256 devices in a mesh: seq: 32 (over y, z), head: 8 (over x, core).
Axes of the slice: x: 4, y: 4, z: 8, core: 2. Of those that a mesh axis runs over, the one named last changes fastest.
Arguments:
- doc_lengths: int32 [256], P(('seq', 'head')), may hold values from 1 to 2688, 24576 in all
- queries: bfloat16 [24576, 8192], P('seq', 'head'), may hold values from -24 to 24
- key_states: bfloat16 [24576, 1024], P('seq', 'head'), may hold values from -24 to 24
- value_states: bfloat16 [24576, 1024], P('seq', 'head'), may hold values from -6 to 6
Outputs:
- attended: bfloat16 [24576, 8192], P('seq', 'head')
The draws below stay inside these ranges and needn't reach their ends.
Inputs may be any that keep to these rules, and one draw needn't show every extreme that they name: `doc_lengths`: the 256 lengths sum to 24576; the largest is exactly 2688.
All inputs are finite; a program needn't handle non-finite values. No bound on the sum of `doc_lengths` on one device may be relied on, other than what follows from the above.
Results may differ from the reference program's by a relative error of at most 0.0028.
Values may be sent and summed in bfloat16 or wider, within the bound.
A program may use at most 64 MiB of HBM per device.

```python
import math
import jax
import jax.numpy as jnp
import numpy as np
from jax import lax

HD = 128
QH = 64
KVH = 8
TILE = 128
GROUP = 8
TOKENS = 24576
DOCS = 256
LONGEST = 2688


def draw_queries(key, part):
    drawn = jnp.clip(jax.random.normal(jax.random.fold_in(key, 1), (TOKENS, QH * HD)), -6.0, 6.0)
    return drawn.astype(jnp.bfloat16)


def draw_key_states(key, part):
    drawn = jnp.clip(jax.random.normal(jax.random.fold_in(key, 2), (TOKENS, KVH * HD)), -6.0, 6.0)
    return drawn.astype(jnp.bfloat16)


def shard_levels(rng, shape, cuts, smallest, top_value):
    def one(dim, shards_of):
        steps = jax.random.uniform(jax.random.fold_in(jax.random.fold_in(rng, 6), dim), (shards_of,), jnp.float32, smallest / len(cuts), top_value / len(cuts))
        return jnp.repeat(jnp.exp(steps), shape[dim] // shards_of).reshape((-1,) + (1,) * (len(shape) - dim - 1))

    gain = one(*cuts[0])
    for cut in cuts[1:]:
        gain = gain * one(*cut)
    return gain


def length_profile(number_of, total, bound, skew):
    weights = [(1 << 20) // math.isqrt(grade ** skew) + 1 for grade in range(2, number_of + 1)]
    rest, counts = total - bound - (number_of - 1), [1] * (number_of - 1)
    while rest > 0:
        candidates = [i for i in range(number_of - 1) if counts[i] < bound]
        whole, remaining = sum([weights[i] for i in candidates]), rest
        for i in candidates:
            extra = min(bound - counts[i], max(1, remaining * weights[i] // whole), rest)
            counts[i] = counts[i] + extra
            rest = rest - extra
    return np.array([bound] + counts)


def ragged(rng, number_of, total, most, skew):
    if number_of == 2:
        one = jax.random.randint(rng, (), max(1, total - most), min(most, total - 1) + 1)
        return jnp.stack([one, total - one])
    tallies = jnp.asarray(length_profile(number_of, total, most, skew), jnp.int32)
    pairs = (number_of - 1) // 2
    giver, taker = tallies[1:1 + 2 * pairs:2], tallies[2:2 + 2 * pairs:2]
    slack = jnp.minimum(giver - 1, most - taker)
    shifted = jax.random.randint(jax.random.fold_in(rng, 1), (pairs,), 0, 1 << 20) % (slack + 1)
    tallies = tallies.at[1:1 + 2 * pairs:2].set(giver - shifted).at[2:2 + 2 * pairs:2].set(taker + shifted)
    return tallies[jax.random.permutation(jax.random.fold_in(rng, 2), number_of)]


def centred(stream_key, shape, deviation, reach, pieces=(), kind=jnp.bfloat16):
    level = shard_levels(stream_key, shape, pieces, -0.22, 0.18) if pieces else 1.0
    values = jax.random.normal(stream_key, shape, jnp.float32) * deviation * level
    return jnp.minimum(jnp.maximum(values, -reach), reach).astype(kind)


def setup_inputs(seed: int = 0) -> dict:
    splits = jax.random.split(jax.random.key(seed), 5)
    return {
        "doc_lengths": ragged(splits[0], DOCS, TOKENS, LONGEST, 2).astype(jnp.int32),
        "queries": draw_queries(jax.random.fold_in(splits[4], 71), 0),
        "key_states": draw_key_states(jax.random.fold_in(splits[4], 71), 0),
        "value_states": centred(splits[3], (TOKENS, KVH * HD), 1.0, 6.0, ((0, 32), (1, 8))),
    }


far_below = -1e+30

def document_start(positions, doc_ends, doc_lengths):
    finished = doc_ends[None, :] <= positions[:, None]
    return lax.optimization_barrier(jnp.sum(jnp.where(finished, doc_lengths[None, :], 0), axis=1)).astype(jnp.int32)

def reference(doc_lengths, queries, key_states, value_states):
    doc_ends = jnp.cumsum(doc_lengths).astype(jnp.int32)
    key_span = LONGEST + TILE
    front_zeros = jnp.zeros((LONGEST, KVH * HD), key_states.dtype)
    padded_keys = jnp.concatenate([front_zeros, key_states], axis=0)
    padded_values = jnp.concatenate([front_zeros, value_states], axis=0)
    score_scale = 1.0 / math.sqrt(HD)

    def one_tile(tile_index):
        first_row = (tile_index * TILE).astype(jnp.int32)
        query_tile = lax.dynamic_slice_in_dim(queries, first_row, TILE, 0).reshape(TILE, KVH, GROUP, HD).astype(jnp.float32)
        key_window = lax.dynamic_slice_in_dim(padded_keys, first_row, key_span, 0).reshape(key_span, KVH, HD).astype(jnp.float32)
        value_window = lax.dynamic_slice_in_dim(padded_values, first_row, key_span, 0).reshape(key_span, KVH, HD).astype(jnp.float32)
        query_pos = first_row + jnp.arange(TILE, dtype=jnp.int32)
        key_pos = first_row - LONGEST + jnp.arange(key_span, dtype=jnp.int32)
        starts = document_start(query_pos, doc_ends, doc_lengths)
        visible = (key_pos[None, :] >= starts[:, None]) & (key_pos[None, :] <= query_pos[:, None])
        scores = jnp.einsum('qhgd,khd->hgqk', query_tile, key_window) * score_scale
        scores = jnp.where(visible, scores, far_below)
        row_max = lax.optimization_barrier(jnp.max(scores, axis=-1, keepdims=True))
        weights = jnp.where(visible, jnp.exp(scores - row_max), 0.0)
        weight_sum = lax.optimization_barrier(jnp.sum(weights, axis=-1, keepdims=True))
        rounded = lax.optimization_barrier(weights.astype(jnp.bfloat16))
        mixed_out = jnp.einsum('hgqk,khd->hgqd', rounded.astype(jnp.float32), value_window) / weight_sum
        return mixed_out.transpose(2, 0, 1, 3).reshape(TILE, QH * HD).astype(jnp.bfloat16)
    all_tiles = lax.map(one_tile, jnp.arange(TOKENS // TILE, dtype=jnp.int32))
    return all_tiles.reshape(TOKENS, QH * HD)
```

```python
import functools
import math

import jax
import jax.numpy as jnp
from jax import lax
from jax.experimental import pallas as pl
from jax.experimental.pallas import tpu as pltpu
from jax.sharding import PartitionSpec as P

HD = 128
TILE = 128
HALF_HEADS = 4
Z = 8
Y = 4
X = 8
LOG2_SCALE = math.log2(math.e) / math.sqrt(HD)
HIDDEN = -1e30
MESH = pl.DeviceIdType.MESH


def exchange_partners(seq, head):
    y, z = seq // Z, seq % Z
    ring_z = [(y * Z + (z + k) % Z, head) for k in range(1, Z)]
    ring_y = [(((y + k) % Y) * Z + z, head) for k in range(1, Y)]
    ring_x = [(seq, (head + k) % X) for k in range(1, X)]
    return ring_z, ring_y, ring_x


def kernel(
    len_ref, q_hbm, k_hbm, v_hbm, out_ref,
    q_buf, k_buf, v_buf, own_len, len_z, len_y, len_x,
    q_extra, k_extra, starts, bias, scores_a, scores_b, row_max, acc,
    load_sems, send_sems, recv_sems, len_send, len_recv,
):
    rows = q_hbm.shape[0]
    half = rows // 2
    tiles = rows // TILE
    devices = 32
    seq = lax.axis_index("seq")
    head = lax.axis_index("head")
    y, z = seq // Z, seq % Z
    following = (lax.rem(seq + 1, devices), head)
    previous = (lax.rem(seq + devices - 1, devices), head)
    ring_z, ring_y, ring_x = exchange_partners(seq, head)

    load_k = pltpu.make_async_copy(k_hbm, k_buf.at[0], load_sems.at[0])
    load_v = pltpu.make_async_copy(v_hbm, v_buf.at[0], load_sems.at[1])
    load_q = pltpu.make_async_copy(q_hbm, q_buf, load_sems.at[2])
    load_k.start()
    load_v.start()
    load_q.start()
    length = jnp.full((1, 1, 128), len_ref[0], jnp.int32)
    own_len[...] = length
    len_z[pl.ds(z, 1)] = length

    barrier = pltpu.get_barrier_semaphore()
    partners = ring_z + ring_y + ring_x + [following, previous]
    for partner in partners:
        pl.semaphore_signal(barrier, inc=1, device_id=partner, device_id_type=MESH)
    pl.semaphore_wait(barrier, len(partners))

    def sends(source, target, partners_of, base):
        return [
            pltpu.make_async_remote_copy(
                src_ref=source, dst_ref=target,
                send_sem=len_send.at[base + n], recv_sem=len_recv.at[base + n],
                device_id=partner, device_id_type=MESH,
            )
            for n, partner in enumerate(partners_of)
        ]

    def hop(slot, part):
        copies = []
        for n, buf in enumerate((k_buf, v_buf)):
            ref = buf.at[slot, pl.ds(part * half, half)]
            if slot == 3:
                target = buf.at[4, pl.ds(0, half)]
            else:
                target = buf.at[slot + 1, pl.ds(part * half, half)]
            copies.append(
                pltpu.make_async_remote_copy(
                    src_ref=ref, dst_ref=target,
                    send_sem=send_sems.at[slot, part, n],
                    recv_sem=recv_sems.at[slot, part, n],
                    device_id=following, device_id_type=MESH,
                )
            )
        return copies

    hops = {(slot, part): hop(slot, part) for slot in range(4) for part in range(slot == 3, 2)}

    def start_hop(slot, part):
        for copy in hops[slot, part]:
            copy.start()

    def wait_hop(slot, part):
        for copy in hops[slot, part]:
            copy.wait_recv()

    z_sends = sends(own_len, len_z.at[pl.ds(z, 1)], ring_z, 0)
    for copy in z_sends:
        copy.start()
    load_k.wait()
    load_v.wait()
    start_hop(0, 0)
    start_hop(0, 1)
    for copy in z_sends:
        copy.wait_recv()
    len_y[pl.ds(y, 1)] = len_z[...].reshape(1, Z, 1, 128)
    y_sends = sends(len_z, len_y.at[y], ring_y, Z - 1)
    for copy in y_sends:
        copy.start()
    wait_hop(0, 0)
    start_hop(1, 0)
    for copy in y_sends:
        copy.wait_recv()
    x_sends = sends(len_y, len_x.at[head], ring_x, Z - 1 + Y - 1)
    for copy in x_sends:
        copy.start()
    len_x[pl.ds(head, 1)] = len_y[...].reshape(1, Y, Z, 1, 128)
    wait_hop(0, 1)
    start_hop(1, 1)
    load_q.wait()
    for copy in x_sends:
        copy.wait_recv()

    lane = lax.broadcasted_iota(jnp.int32, (1, 128), 1)

    def add_lengths(n, ends):
        low, high = ends
        for m in range(X):
            length_row = len_x[m, n // Z, n % Z]
            doc = n * X + m
            low = low + jnp.where(lane >= doc, length_row, 0)
            high = high + jnp.where(lane + 128 >= doc, length_row, 0)
        return low, high

    zero_row = jnp.zeros((1, 128), jnp.int32)
    low, high = lax.fori_loop(0, devices, add_lengths, (zero_row, zero_row))
    ends = jnp.concatenate([low, high], axis=1)
    first = seq * rows
    doc_first = jnp.max(jnp.where(ends <= first, ends, 0), axis=1, keepdims=True)
    doc_end = jnp.min(jnp.where(ends > first, ends, 1 << 30), axis=1, keepdims=True)
    column = lax.broadcasted_iota(jnp.int32, (TILE, 128), 0)
    lanes = lax.broadcasted_iota(jnp.int32, (TILE, 128), 1)

    def tile_masks(tile, carry):
        at = pl.ds(tile * TILE, TILE)
        position = first + tile * TILE + column
        done = jnp.where(ends <= position[:, :1], ends, 0)
        starts[at, :] = jnp.broadcast_to(jnp.max(done, axis=1, keepdims=True), (TILE, 128)) - first
        later = jnp.where(position >= doc_end, 1.0, 0.0)
        q_extra[at, :] = jnp.where(lanes == 0, later, jnp.where(lanes == 1, 1.0, 0.0)).astype(jnp.bfloat16)
        for slot in range(1, 5):
            token = position - slot * rows
            before = jnp.where(token < doc_first, HIDDEN, 0.0)
            k_extra[slot, at, :] = jnp.where(
                lanes == 0, HIDDEN, jnp.where(lanes == 1, before, 0.0)
            ).astype(jnp.bfloat16)
        return carry

    lax.fori_loop(0, tiles, tile_masks, 0)

    def queries_of(tile, group, own):
        at = pl.ds(tile * TILE, TILE)
        parts = []
        for n in range(HALF_HEADS):
            cols = pl.ds((group * HALF_HEADS + n) * HD, HD)
            parts.append(q_buf[at, cols])
        stacked = jnp.concatenate(parts, axis=0)
        if own:
            return stacked
        extra = jnp.concatenate([q_extra[at, :]] * HALF_HEADS, axis=0)
        return jnp.concatenate([stacked, extra], axis=1)

    def attend(slot, tile_range, key0, width, hooks):
        own = slot == 0
        keys_at = pl.ds(key0, width)
        extra0 = half if slot == 4 else 0

        def score(tile, group, target):
            keys = k_buf[slot, keys_at, :]
            if not own:
                extra = k_extra[slot, pl.ds(extra0 + key0, width), :]
                keys = jnp.concatenate([keys, extra], axis=1)
            target[:, pl.ds(0, width)] = lax.dot_general(
                queries_of(tile, group, own), keys, (((1,), (1,)), ((), ())),
                preferred_element_type=jnp.float32,
            )

        def combine(tile, group, source):
            parts, shrinks = [], []
            for n in range(HALF_HEADS):
                s = source[pl.ds(n * TILE, TILE), pl.ds(0, width)]
                at = pl.ds(n * TILE, TILE)
                if own:
                    s = s + bias[:, pl.ds(0, width)]
                    top = jnp.max(s, axis=1, keepdims=True)
                else:
                    old = row_max[tile, group, at, :]
                    top = jnp.maximum(old, jnp.max(s, axis=1, keepdims=True))
                    shrinks.append(jnp.exp2((old - top) * LOG2_SCALE))
                row_max[tile, group, at, :] = jnp.broadcast_to(top, (TILE, 128))
                if not own:
                    top = jnp.concatenate([top] * (width // 128), axis=1)
                parts.append(jnp.exp2((s - top) * LOG2_SCALE).astype(jnp.bfloat16))
            values = jnp.concatenate(
                [v_buf[slot, keys_at, :], jnp.ones((width, 128), jnp.bfloat16)], axis=1
            )
            update = jnp.dot(
                jnp.concatenate(parts, axis=0), values, preferred_element_type=jnp.float32
            )
            if own:
                acc[tile, group] = update
            else:
                shrink = jnp.concatenate(shrinks, axis=0)
                shrink = jnp.concatenate([shrink, shrink], axis=1)
                acc[tile, group] = acc[tile, group] * shrink + update

        begin, end = tile_range
        score(begin, 0, scores_a)

        def step(tile, carry):
            for at_tile, hook in hooks.items():
                pl.when(tile == at_tile)(hook)
            if own:
                token = lax.broadcasted_iota(jnp.int32, (TILE, width), 1) + key0
                mine = tile * TILE + lax.broadcasted_iota(jnp.int32, (TILE, width), 0)
                begins = starts[pl.ds(tile * TILE, TILE), :]
                begins = jnp.concatenate([begins] * (width // 128), axis=1)
                seen = (token >= begins) & (token <= mine)
                bias[:, pl.ds(0, width)] = jnp.where(seen, 0.0, HIDDEN)
            score(tile, 1, scores_b)
            combine(tile, 0, scores_a)
            score(jnp.minimum(tile + 1, end - 1), 0, scores_a)
            combine(tile, 1, scores_b)
            return carry

        lax.fori_loop(begin, end, step, 0)

    def forward(slot, part):
        def run():
            wait_hop(slot, part)
            if (slot + 1, part) in hops:
                start_hop(slot + 1, part)
        return run

    for pair in range(tiles // 2):
        attend(0, (2 * pair, 2 * pair + 2), 0, 2 * TILE * (pair + 1), {})
    forward(1, 0)()
    attend(1, (0, tiles), 0, rows, {4: forward(1, 1)})
    attend(2, (0, tiles), 0, rows, {4: forward(2, 0)})
    forward(2, 1)()
    attend(3, (0, tiles), 0, rows, {})
    forward(3, 1)()
    attend(4, (0, tiles // 2), 0, half, {})

    def finish(tile, carry):
        for group in range(2):
            done = acc[tile, group]
            done = (done[:, :HD] / done[:, HD:]).astype(jnp.bfloat16)
            for n in range(HALF_HEADS):
                cols = pl.ds((group * HALF_HEADS + n) * HD, HD)
                out_ref[pl.ds(tile * TILE, TILE), cols] = done[n * TILE : (n + 1) * TILE]
        return carry

    lax.fori_loop(0, tiles, finish, 0)
    for copy in z_sends + y_sends + x_sends:
        copy.wait_send()
    for copies in hops.values():
        for copy in copies:
            copy.wait_send()


def body(doc_lengths, queries, key_states, value_states):
    rows, cols = queries.shape
    tiles = rows // TILE
    group_rows = HALF_HEADS * TILE
    vmem = pltpu.VMEM
    any_space = pl.BlockSpec(memory_space=pl.ANY)
    return pl.pallas_call(
        kernel,
        out_shape=jax.ShapeDtypeStruct((rows, cols), jnp.bfloat16),
        in_specs=[pl.BlockSpec(memory_space=pltpu.SMEM), any_space, any_space, any_space],
        out_specs=pl.BlockSpec(memory_space=pltpu.VMEM),
        scratch_shapes=[
            vmem((rows, cols), jnp.bfloat16),
            vmem((5, rows, HD), jnp.bfloat16),
            vmem((5, rows, HD), jnp.bfloat16),
            vmem((1, 1, 128), jnp.int32),
            vmem((Z, 1, 128), jnp.int32),
            vmem((Y, Z, 1, 128), jnp.int32),
            vmem((X, Y, Z, 1, 128), jnp.int32),
            vmem((rows, 128), jnp.bfloat16),
            vmem((5, rows, 128), jnp.bfloat16),
            vmem((rows, 128), jnp.int32),
            vmem((TILE, rows), jnp.float32),
            vmem((group_rows, rows), jnp.float32),
            vmem((group_rows, rows), jnp.float32),
            vmem((tiles, 2, group_rows, 128), jnp.float32),
            vmem((tiles, 2, group_rows, 2 * HD), jnp.float32),
            pltpu.SemaphoreType.DMA((3,)),
            pltpu.SemaphoreType.DMA((4, 2, 2)),
            pltpu.SemaphoreType.DMA((4, 2, 2)),
            pltpu.SemaphoreType.DMA((Z + Y + X - 3,)),
            pltpu.SemaphoreType.DMA((Z + Y + X - 3,)),
        ],
        compiler_params=pltpu.CompilerParams(
            collective_id=0, has_side_effects=True, vmem_limit_bytes=56 * 1024 * 1024
        ),
    )(doc_lengths, queries, key_states, value_states)


def solution(mesh):
    return jax.shard_map(
        body,
        mesh=mesh,
        in_specs=(P(("seq", "head")), P("seq", "head"), P("seq", "head"), P("seq", "head")),
        out_specs=P("seq", "head"),
        check_vma=False,
    )
```

```python
import functools
import math

import jax
import jax.numpy as jnp
from jax import lax
from jax.experimental import pallas as pl
from jax.experimental.pallas import tpu as pltpu
from jax.sharding import PartitionSpec as P

HD = 128
TILE = 128
HALF_HEADS = 4
SEQ = 32
HEADS = 8
LOG2_SCALE = math.log2(math.e) / math.sqrt(HD)
HIDDEN = -1e30
MESH = pl.DeviceIdType.MESH


def kernel(
    len_ref, q_hbm, k_hbm, v_hbm, acc,
    q_buf, k_buf, v_buf, own_len, len_seq, len_all,
    q_extra, k_extra, starts, bias, scores_a, scores_b, row_max,
    load_sems, send_sems, recv_sems, len_send, len_recv,
):
    rows = q_hbm.shape[0]
    half = rows // 2
    tiles = rows // TILE
    seq = lax.axis_index("seq")
    head = lax.axis_index("head")
    along_seq = [(lax.rem(seq + k, SEQ), head) for k in range(1, SEQ)]
    along_head = [(seq, lax.rem(head + k, HEADS)) for k in range(1, HEADS)]
    following = along_seq[0]

    load_k = pltpu.make_async_copy(k_hbm, k_buf.at[0], load_sems.at[0])
    load_v = pltpu.make_async_copy(v_hbm, v_buf.at[0], load_sems.at[1])
    load_q = pltpu.make_async_copy(q_hbm, q_buf, load_sems.at[2])
    load_k.start()
    load_v.start()
    load_q.start()
    length = jnp.full((1, 1, 128), len_ref[0], jnp.int32)
    own_len[...] = length
    len_seq[pl.ds(seq, 1)] = length

    barrier = pltpu.get_barrier_semaphore()
    partners = along_seq + along_head
    for partner in partners:
        pl.semaphore_signal(barrier, inc=1, device_id=partner, device_id_type=MESH)
    pl.semaphore_wait(barrier, len(partners))

    def sends(source, target, partners_of, base):
        return [
            pltpu.make_async_remote_copy(
                src_ref=source, dst_ref=target,
                send_sem=len_send.at[base + n], recv_sem=len_recv.at[base + n],
                device_id=partner, device_id_type=MESH,
            )
            for n, partner in enumerate(partners_of)
        ]

    def hop(slot, part):
        copies = []
        for n, buf in enumerate((k_buf, v_buf)):
            ref = buf.at[slot, pl.ds(part * half, half)]
            if slot == 3:
                target = buf.at[4, pl.ds(0, half)]
            else:
                target = buf.at[slot + 1, pl.ds(part * half, half)]
            copies.append(
                pltpu.make_async_remote_copy(
                    src_ref=ref, dst_ref=target,
                    send_sem=send_sems.at[slot, part, n],
                    recv_sem=recv_sems.at[slot, part, n],
                    device_id=following, device_id_type=MESH,
                )
            )
        return copies

    hops = {(slot, part): hop(slot, part) for slot in range(4) for part in range(slot == 3, 2)}

    def start_hop(slot, part):
        for copy in hops[slot, part]:
            copy.start()

    def wait_hop(slot, part):
        for copy in hops[slot, part]:
            copy.wait_recv()

    seq_sends = sends(own_len, len_seq.at[pl.ds(seq, 1)], along_seq, 0)
    for copy in seq_sends:
        copy.start()
    load_k.wait()
    load_v.wait()
    start_hop(0, 0)
    start_hop(0, 1)
    for copy in seq_sends:
        copy.wait_recv()
    head_sends = sends(len_seq, len_all.at[head], along_head, SEQ - 1)
    for copy in head_sends:
        copy.start()
    len_all[pl.ds(head, 1)] = len_seq[...].reshape(1, SEQ, 1, 128)
    wait_hop(0, 0)
    start_hop(1, 0)
    load_q.wait()
    for copy in head_sends:
        copy.wait_recv()

    lane = lax.broadcasted_iota(jnp.int32, (1, 128), 1)

    def add_lengths(n, ends):
        low, high = ends
        for m in range(HEADS):
            length_row = len_all[m, n]
            doc = n * HEADS + m
            low = low + jnp.where(lane >= doc, length_row, 0)
            high = high + jnp.where(lane + 128 >= doc, length_row, 0)
        return low, high

    zero_row = jnp.zeros((1, 128), jnp.int32)
    low, high = lax.fori_loop(0, SEQ, add_lengths, (zero_row, zero_row))
    ends = jnp.concatenate([low, high], axis=1)
    first = seq * rows
    doc_first = jnp.max(jnp.where(ends <= first, ends, 0), axis=1, keepdims=True)
    doc_end = jnp.min(jnp.where(ends > first, ends, 1 << 30), axis=1, keepdims=True)
    column = lax.broadcasted_iota(jnp.int32, (TILE, 128), 0)
    lanes = lax.broadcasted_iota(jnp.int32, (TILE, 128), 1)

    def tile_masks(tile, carry):
        at = pl.ds(tile * TILE, TILE)
        position = first + tile * TILE + column
        done = jnp.where(ends <= position[:, :1], ends, 0)
        starts[at, :] = jnp.broadcast_to(jnp.max(done, axis=1, keepdims=True), (TILE, 128)) - first
        later = jnp.where(position >= doc_end, 1.0, 0.0)
        q_extra[at, :] = jnp.where(lanes == 0, later, jnp.where(lanes == 1, 1.0, 0.0)).astype(jnp.bfloat16)
        for slot in range(1, 5):
            token = position - slot * rows
            before = jnp.where(token < doc_first, HIDDEN, 0.0)
            k_extra[slot, at, :] = jnp.where(
                lanes == 0, HIDDEN, jnp.where(lanes == 1, before, 0.0)
            ).astype(jnp.bfloat16)
        return carry

    lax.fori_loop(0, tiles, tile_masks, 0)

    def stacked_queries(tile, group, own):
        at = pl.ds(tile * TILE, TILE)
        parts = []
        for n in range(HALF_HEADS):
            cols = pl.ds((group * HALF_HEADS + n) * HD, HD)
            parts.append(q_buf[at, cols])
        stacked = jnp.concatenate(parts, axis=0)
        if own:
            return stacked
        extra = jnp.concatenate([q_extra[at, :]] * HALF_HEADS, axis=0)
        return jnp.concatenate([stacked, extra], axis=1)

    def score(slot, keys_at, extra_at, tile, group, target):
        own = extra_at is None
        keys = k_buf[slot, keys_at, :]
        if not own:
            keys = jnp.concatenate([keys, k_extra[slot, extra_at, :]], axis=1)
        target[:, pl.ds(0, keys.shape[0])] = lax.dot_general(
            stacked_queries(tile, group, own), keys, (((1,), (1,)), ((), ())),
            preferred_element_type=jnp.float32,
        )

    def combine(slot, keys_at, own, tile, group, source):
        width = keys_at.size
        parts, shrinks = [], []
        for n in range(HALF_HEADS):
            at = pl.ds(n * TILE, TILE)
            s = source[at, pl.ds(0, width)]
            if own:
                s = s + bias[:, pl.ds(0, width)]
                top = jnp.max(s, axis=1, keepdims=True)
            else:
                old = row_max[tile, group, at, :]
                top = jnp.maximum(old, jnp.max(s, axis=1, keepdims=True))
                shrinks.append(jnp.exp2((old - top) * LOG2_SCALE))
            row_max[tile, group, at, :] = jnp.broadcast_to(top, (TILE, 128))
            if not own:
                top = jnp.concatenate([top] * (width // 128), axis=1)
            parts.append(jnp.exp2((s - top) * LOG2_SCALE).astype(jnp.bfloat16))
        values = jnp.concatenate(
            [v_buf[slot, keys_at, :], jnp.ones((width, 128), jnp.bfloat16)], axis=1
        )
        update = jnp.dot(
            jnp.concatenate(parts, axis=0), values, preferred_element_type=jnp.float32
        )
        if own:
            acc[tile, group] = update
        else:
            shrink = jnp.concatenate(shrinks, axis=0)
            shrink = jnp.concatenate([shrink, shrink], axis=1)
            acc[tile, group] = acc[tile, group] * shrink + update

    for pair in range(tiles // 2):
        width = 2 * TILE * (pair + 1)
        keys_at = pl.ds(0, width)
        score(0, keys_at, None, 2 * pair, 0, scores_a)
        for tile in (2 * pair, 2 * pair + 1):
            token = lax.broadcasted_iota(jnp.int32, (TILE, width), 1)
            mine = tile * TILE + lax.broadcasted_iota(jnp.int32, (TILE, width), 0)
            begins = starts[pl.ds(tile * TILE, TILE), :]
            begins = jnp.concatenate([begins] * (width // 128), axis=1)
            seen = (token >= begins) & (token <= mine)
            bias[:, pl.ds(0, width)] = jnp.where(seen, 0.0, HIDDEN)
            score(0, keys_at, None, tile, 1, scores_b)
            combine(0, keys_at, True, tile, 0, scores_a)
            if tile == 2 * pair:
                score(0, keys_at, None, tile + 1, 0, scores_a)
            combine(0, keys_at, True, tile, 1, scores_b)

    def arrived(slot, part):
        wait_hop(slot, part)
        if (slot + 1, part) in hops:
            start_hop(slot + 1, part)

    arrived(0, 1)
    whole = pl.ds(0, rows)
    pairs = tiles // 2
    trips = 3 * pairs

    def place(trip):
        return trip // pairs + 1, trip % pairs * 2

    def trip_body(trip, carry):
        for when, slot, part in ((0, 1, 0), (1, 1, 1), (4, 2, 0), (5, 2, 1)):
            pl.when(trip == when)(functools.partial(arrived, slot, part))
        slot, tile = place(trip)
        next_slot, next_tile = place(jnp.minimum(trip + 1, trips - 1))
        score(slot, whole, whole, tile, 1, scores_b)
        combine(slot, whole, False, tile, 0, scores_a)
        score(slot, whole, whole, tile + 1, 0, scores_a)
        combine(slot, whole, False, tile, 1, scores_b)
        score(slot, whole, whole, tile + 1, 1, scores_b)
        combine(slot, whole, False, tile + 1, 0, scores_a)
        score(next_slot, whole, whole, next_tile, 0, scores_a)
        combine(slot, whole, False, tile + 1, 1, scores_b)
        return carry

    score(1, whole, whole, 0, 0, scores_a)
    lax.fori_loop(0, trips, trip_body, 0)
    arrived(3, 1)
    for tile in range(tiles // 2):
        keys_at = pl.ds(tile * TILE, half - tile * TILE)
        extra_at = pl.ds(half + tile * TILE, half - tile * TILE)
        for group, target in enumerate((scores_a, scores_b)):
            score(4, keys_at, extra_at, tile, group, target)
            combine(4, keys_at, False, tile, group, target)

    for copy in seq_sends + head_sends:
        copy.wait_send()
    for copies in hops.values():
        for copy in copies:
            copy.wait_send()


def finish(acc, out_hbm, out_buf, sems):
    copies = []
    for tile in range(acc.shape[0]):
        at = pl.ds(tile * TILE, TILE)
        for group in range(2):
            done = acc[tile, group]
            done = (done[:, :HD] / done[:, HD:]).astype(jnp.bfloat16)
            for n in range(HALF_HEADS):
                cols = pl.ds((group * HALF_HEADS + n) * HD, HD)
                out_buf[at, cols] = done[n * TILE : (n + 1) * TILE]
        copy = pltpu.make_async_copy(out_buf.at[at], out_hbm.at[at], sems.at[tile])
        copy.start()
        copies.append(copy)
    for copy in copies:
        copy.wait()


def body(doc_lengths, queries, key_states, value_states):
    rows, cols = queries.shape
    tiles = rows // TILE
    group_rows = HALF_HEADS * TILE
    vmem = pltpu.VMEM
    any_space = pl.BlockSpec(memory_space=pl.ANY)
    acc = pl.pallas_call(
        kernel,
        out_shape=vmem((tiles, 2, group_rows, 2 * HD), jnp.float32),
        in_specs=[pl.BlockSpec(memory_space=pltpu.SMEM), any_space, any_space, any_space],
        out_specs=pl.BlockSpec(memory_space=pltpu.VMEM),
        scratch_shapes=[
            vmem((rows, cols), jnp.bfloat16),
            vmem((5, rows, HD), jnp.bfloat16),
            vmem((5, rows, HD), jnp.bfloat16),
            vmem((1, 1, 128), jnp.int32),
            vmem((SEQ, 1, 128), jnp.int32),
            vmem((HEADS, SEQ, 1, 128), jnp.int32),
            vmem((rows, 128), jnp.bfloat16),
            vmem((5, rows, 128), jnp.bfloat16),
            vmem((rows, 128), jnp.int32),
            vmem((TILE, rows), jnp.float32),
            vmem((group_rows, rows), jnp.float32),
            vmem((group_rows, rows), jnp.float32),
            vmem((tiles, 2, group_rows, 128), jnp.float32),
            pltpu.SemaphoreType.DMA((3,)),
            pltpu.SemaphoreType.DMA((4, 2, 2)),
            pltpu.SemaphoreType.DMA((4, 2, 2)),
            pltpu.SemaphoreType.DMA((SEQ + HEADS - 2,)),
            pltpu.SemaphoreType.DMA((SEQ + HEADS - 2,)),
        ],
        compiler_params=pltpu.CompilerParams(
            collective_id=0, has_side_effects=True, vmem_limit_bytes=48 * 1024 * 1024
        ),
    )(doc_lengths, queries, key_states, value_states)
    return pl.pallas_call(
        finish,
        out_shape=jax.ShapeDtypeStruct((rows, cols), jnp.bfloat16),
        in_specs=[pl.BlockSpec(memory_space=pltpu.VMEM)],
        out_specs=any_space,
        scratch_shapes=[vmem((rows, cols), jnp.bfloat16), pltpu.SemaphoreType.DMA((tiles,))],
        compiler_params=pltpu.CompilerParams(vmem_limit_bytes=12 * 1024 * 1024),
    )(acc)


def solution(mesh):
    return jax.shard_map(
        body,
        mesh=mesh,
        in_specs=(P(("seq", "head")), P("seq", "head"), P("seq", "head"), P("seq", "head")),
        out_specs=P("seq", "head"),
        check_vma=False,
    )
```

```python
import functools
import math

import jax
import jax.numpy as jnp
from jax import lax
from jax.experimental import pallas as pl
from jax.experimental.pallas import tpu as pltpu
from jax.sharding import PartitionSpec as P

HD = 128
TILE = 128
HALF_HEADS = 4
SEQ = 32
RING = 8
HEADS = 8
LOG2_SCALE = math.log2(math.e) / math.sqrt(HD)
HIDDEN = -1e30
MESH = pl.DeviceIdType.MESH


def stacked_queries(q_buf, q_extra, tile, group):
    at = pl.ds(tile * TILE, TILE)
    parts = []
    for n in range(HALF_HEADS):
        cols = pl.ds((group * HALF_HEADS + n) * HD, HD)
        parts.append(q_buf[at, cols])
    stacked = jnp.concatenate(parts, axis=0)
    if q_extra is None:
        return stacked
    extra = jnp.concatenate([q_extra[at, :]] * HALF_HEADS, axis=0)
    return jnp.concatenate([stacked, extra], axis=1)


def dot_keys(queries, keys):
    return lax.dot_general(
        queries, keys, (((1,), (1,)), ((), ())), preferred_element_type=jnp.float32
    )


def weigh(scores, values, bias, old_max):
    width = values.shape[0]
    parts, tops, shrinks = [], [], []
    for n in range(HALF_HEADS):
        at = pl.ds(n * TILE, TILE)
        s = scores[at, pl.ds(0, width)]
        if bias is not None:
            s = s + bias[:, pl.ds(0, width)]
        top = jnp.max(s, axis=1, keepdims=True)
        if old_max is None:
            tops.append(jnp.broadcast_to(top, (TILE, 128)))
        else:
            old = old_max[at, :]
            top = jnp.maximum(old, top)
            tops.append(top)
            shrinks.append(jnp.exp2((old - top) * LOG2_SCALE))
            top = jnp.concatenate([top] * (width // 128), axis=1)
        parts.append(jnp.exp2((s - top) * LOG2_SCALE).astype(jnp.bfloat16))
    values = jnp.concatenate([values, jnp.ones((width, 128), jnp.bfloat16)], axis=1)
    update = jnp.dot(
        jnp.concatenate(parts, axis=0), values, preferred_element_type=jnp.float32
    )
    return update, tops, shrinks


def both_halves(shrinks):
    shrink = jnp.concatenate(shrinks, axis=0)
    return jnp.concatenate([shrink, shrink], axis=1)


def kernel(
    len_ref, q_hbm, k_hbm, v_hbm,
    acc, row_max, q_buf, k_buf, v_buf, q_extra, k_extra, crossing,
    relay_buf, own_len, len_seq, len_all, starts, bias,
    own_scores_0, own_scores_1, own_scores_2, scores_a, scores_b,
    load_sems, send_sems, recv_sems, len_send, len_recv,
):
    rows = q_hbm.shape[0]
    half = rows // 2
    tiles = rows // TILE
    own_scores = (own_scores_0, own_scores_1, own_scores_2)
    seq = lax.axis_index("seq")
    head = lax.axis_index("head")
    along_seq = [(lax.rem(seq + k, SEQ), head) for k in range(1, SEQ)]
    along_head = [(seq, lax.rem(head + k, HEADS)) for k in range(1, HEADS)]
    following = along_seq[0]
    ahead = lax.rem(seq + 4, SEQ)
    relay = (ahead // RING * RING + lax.rem(seq + RING - 2, RING), head)
    relayed = (seq // RING * RING + lax.rem(seq + RING - 2, RING), head)

    load_k = pltpu.make_async_copy(k_hbm, k_buf.at[0], load_sems.at[0])
    load_v = pltpu.make_async_copy(v_hbm, v_buf.at[0], load_sems.at[1])
    load_q = pltpu.make_async_copy(q_hbm, q_buf, load_sems.at[2])
    load_k.start()
    load_v.start()
    load_q.start()
    length = jnp.full((1, 1, 128), len_ref[0], jnp.int32)
    own_len[...] = length
    len_seq[pl.ds(seq, 1)] = length

    barrier = pltpu.get_barrier_semaphore()
    partners = along_seq + along_head
    for partner in partners:
        pl.semaphore_signal(barrier, inc=1, device_id=partner, device_id_type=MESH)
    pl.semaphore_wait(barrier, len(partners))

    def sends(source, target, partners_of, base):
        return [
            pltpu.make_async_remote_copy(
                src_ref=source, dst_ref=target,
                send_sem=len_send.at[base + n], recv_sem=len_recv.at[base + n],
                device_id=partner, device_id_type=MESH,
            )
            for n, partner in enumerate(partners_of)
        ]

    def hop(slot, part):
        at = pl.ds(part * half, half)
        if slot < 3:
            pairs = [(buf.at[slot, at], buf.at[slot + 1, at]) for buf in (k_buf, v_buf)]
            target = following
        elif part == 0:
            late = pl.ds(half, half)
            pairs = [(buf.at[0, late], relay_buf.at[n]) for n, buf in enumerate((k_buf, v_buf))]
            target = relay
        else:
            early = pl.ds(0, half)
            pairs = [(relay_buf.at[n], buf.at[4, early]) for n, buf in enumerate((k_buf, v_buf))]
            target = relayed
        return [
            pltpu.make_async_remote_copy(
                src_ref=source, dst_ref=held,
                send_sem=send_sems.at[slot, part, n], recv_sem=recv_sems.at[slot, part, n],
                device_id=target, device_id_type=MESH,
            )
            for n, (source, held) in enumerate(pairs)
        ]

    hops = {(slot, part): hop(slot, part) for slot in range(4) for part in range(2)}

    def start_hop(slot, part):
        for copy in hops[slot, part]:
            copy.start()

    def wait_hop(slot, part):
        for copy in hops[slot, part]:
            copy.wait_recv()

    def arrived(slot, part):
        wait_hop(slot, part)
        if slot < 2:
            start_hop(slot + 1, part)

    seq_sends = sends(own_len, len_seq.at[pl.ds(seq, 1)], along_seq, 0)
    for copy in seq_sends:
        copy.start()
    load_k.wait()
    load_v.wait()
    start_hop(0, 0)
    start_hop(0, 1)
    start_hop(3, 0)
    load_q.wait()
    for tile in range(tiles):
        pair = tile // 2
        for group in range(2):
            own_scores[pair][tile % 2, group] = dot_keys(
                stacked_queries(q_buf, None, tile, group),
                k_buf[0, pl.ds(0, 2 * TILE * (pair + 1)), :],
            )
    for copy in seq_sends:
        copy.wait_recv()
    head_sends = sends(len_seq, len_all.at[head], along_head, SEQ - 1)
    for copy in head_sends:
        copy.start()
    len_all[pl.ds(head, 1)] = len_seq[...].reshape(1, SEQ, 1, 128)
    arrived(0, 0)
    for copy in head_sends:
        copy.wait_recv()
    arrived(0, 1)

    lane = lax.broadcasted_iota(jnp.int32, (1, 128), 1)

    def add_lengths(n, ends):
        low, high = ends
        for m in range(HEADS):
            length_row = len_all[m, n]
            doc = n * HEADS + m
            low = low + jnp.where(lane >= doc, length_row, 0)
            high = high + jnp.where(lane + 128 >= doc, length_row, 0)
        return low, high

    zero_row = jnp.zeros((1, 128), jnp.int32)
    low, high = lax.fori_loop(0, SEQ, add_lengths, (zero_row, zero_row))
    first = seq * rows
    ends = (jnp.concatenate([low, high], axis=1) - first).astype(jnp.float32)
    far = float(1 << 24)
    doc_first = jnp.max(
        jnp.maximum(jnp.where(ends <= 0, ends, -far), (0 - first).astype(jnp.float32)),
        axis=1, keepdims=True,
    )
    doc_end = jnp.min(jnp.where(ends > 0, ends, far), axis=1, keepdims=True)
    crossing[0:1, :] = jnp.broadcast_to(doc_first, (1, 128))
    crossing[1:2, :] = jnp.broadcast_to(doc_end, (1, 128))
    column = lax.broadcasted_iota(jnp.int32, (TILE, 128), 0).astype(jnp.float32)
    lanes = lax.broadcasted_iota(jnp.int32, (TILE, 128), 1)
    unseen_lane = jnp.where(lanes == 0, HIDDEN, 0.0)
    one_lane = jnp.where(lanes == 1, 1.0, 0.0)
    for tile in range(tiles):
        at = pl.ds(tile * TILE, TILE)
        position = column + float(tile * TILE)
        done = jnp.where(ends <= position[:, :1], ends, -far)
        starts[at, :] = jnp.broadcast_to(jnp.max(done, axis=1, keepdims=True), (TILE, 128))
        later = (lanes == 0) & (position >= doc_end)
        q_extra[at, :] = jnp.where(later, 1.0, one_lane).astype(jnp.bfloat16)
        for slot in range(1, 5):
            before = (lanes == 1) & (position < doc_first + float(slot * rows))
            k_extra[slot, at, :] = jnp.where(before, HIDDEN, unseen_lane).astype(jnp.bfloat16)

    def score(slot, keys_at, extra_at, tile, group, target):
        keys = jnp.concatenate([k_buf[slot, keys_at, :], k_extra[slot, extra_at, :]], axis=1)
        target[:, pl.ds(0, keys_at.size)] = dot_keys(
            stacked_queries(q_buf, q_extra, tile, group), keys
        )

    def combine(slot, keys_at, tile, group, source):
        update, tops, shrinks = weigh(
            source, v_buf[slot, keys_at, :], None, row_max.at[tile, group]
        )
        for n, top in enumerate(tops):
            row_max[tile, group, pl.ds(n * TILE, TILE), :] = top
        acc[tile, group] = acc[tile, group] * both_halves(shrinks) + update

    for tile in range(tiles):
        pair = tile // 2
        width = 2 * TILE * (pair + 1)
        token = lax.broadcasted_iota(jnp.int32, (TILE, width), 1)
        mine = tile * TILE + lax.broadcasted_iota(jnp.int32, (TILE, width), 0)
        begins = starts[pl.ds(tile * TILE, TILE), :]
        begins = jnp.concatenate([begins] * (width // 128), axis=1)
        seen = (token.astype(jnp.float32) >= begins) & (token <= mine)
        bias[:, pl.ds(0, width)] = jnp.where(seen, 0.0, HIDDEN)
        for group in range(2):
            update, tops, _ = weigh(
                own_scores[pair].at[tile % 2, group], v_buf[0, pl.ds(0, width), :], bias, None
            )
            for n, top in enumerate(tops):
                row_max[tile, group, pl.ds(n * TILE, TILE), :] = top
            acc[tile, group] = update
        if tile == 1:
            wait_hop(3, 0)
            start_hop(3, 1)

    whole = pl.ds(0, rows)
    step = 3
    blocks = tiles // step
    trips = 2 * blocks
    buffers = (scores_a, scores_b)

    def place(trip):
        return trip // blocks + 1, trip % blocks * step

    def trip_body(trip, carry):
        for when, slot, part in ((0, 1, 0), (1, 1, 1), (3, 2, 0)):
            pl.when(trip == when)(functools.partial(arrived, slot, part))
        slot, tile = place(trip)
        next_slot, next_tile = place(jnp.minimum(trip + 1, trips - 1))
        units = [(slot, tile + n, group) for n in range(step) for group in range(2)]
        for n, (_, at_tile, group) in enumerate(units):
            ahead_slot, ahead_tile, ahead_group = (units + [(next_slot, next_tile, 0)])[n + 1]
            score(ahead_slot, whole, whole, ahead_tile, ahead_group, buffers[1 - n % 2])
            combine(slot, whole, at_tile, group, buffers[n % 2])
        return carry

    score(1, whole, whole, 0, 0, scores_a)
    lax.fori_loop(0, trips, trip_body, 0)
    wait_hop(3, 1)
    for tile in range(tiles // 2):
        keys_at = pl.ds(tile * TILE, half - tile * TILE)
        extra_at = pl.ds(half + tile * TILE, half - tile * TILE)
        for group, target in enumerate(buffers):
            score(4, keys_at, extra_at, tile, group, target)
            combine(4, keys_at, tile, group, target)
    wait_hop(2, 1)
    for copy in seq_sends + head_sends:
        copy.wait_send()
    for copies in hops.values():
        for copy in copies:
            copy.wait_send()


def tail(
    acc, row_max, q_buf, k_buf, v_buf, q_extra, k_extra, crossing, out_hbm,
    out_buf, scores_a, scores_b, sems,
):
    rows = q_buf.shape[0]
    tiles = rows // TILE
    slot = 3
    third = rows // 3
    doc_first = jnp.max(crossing[0:1, :]).astype(jnp.int32)
    doc_end = jnp.max(crossing[1:2, :]).astype(jnp.int32)
    first_key = jnp.maximum(doc_first + slot * rows, 0)
    thirds = 3 - jnp.minimum(first_key // third, 3)
    seeing = (jnp.minimum(doc_end, rows) + 2 * TILE - 1) // (2 * TILE)
    seeing = jnp.where(thirds > 0, seeing, 0)

    def out_copy(tile):
        at = pl.ds(tile * TILE, TILE)
        return pltpu.make_async_copy(out_buf.at[at], out_hbm.at[at], sems.at[tile])

    def put(tile, group, total):
        total = (total[:, :HD] / total[:, HD:]).astype(jnp.bfloat16)
        for n in range(HALF_HEADS):
            cols = pl.ds((group * HALF_HEADS + n) * HD, HD)
            out_buf[pl.ds(tile * TILE, TILE), cols] = total[n * TILE : (n + 1) * TILE]

    def finish(tile, carry):
        for group in range(2):
            put(tile, group, acc[tile, group])
        out_copy(tile).start()
        return carry

    lax.fori_loop(2 * seeing, tiles, finish, 0)

    for count in range(1, 4):
        width = count * third
        keys_at = pl.ds(rows - width, width)

        def score(tile, group, target, keys_at=keys_at, width=width):
            keys = jnp.concatenate([k_buf[slot, keys_at, :], k_extra[slot, keys_at, :]], axis=1)
            target[:, pl.ds(0, width)] = dot_keys(
                stacked_queries(q_buf, q_extra, tile, group), keys
            )

        def combine(tile, group, source, keys_at=keys_at):
            update, _, shrinks = weigh(
                source, v_buf[slot, keys_at, :], None, row_max.at[tile, group]
            )
            put(tile, group, acc[tile, group] * both_halves(shrinks) + update)

        def trip(n, carry, score=score, combine=combine):
            tile = 2 * n
            score(tile, 1, scores_b)
            combine(tile, 0, scores_a)
            score(tile + 1, 0, scores_a)
            combine(tile, 1, scores_b)
            score(tile + 1, 1, scores_b)
            combine(tile + 1, 0, scores_a)
            score(jnp.minimum(tile + 2, tiles - 1), 0, scores_a)
            combine(tile + 1, 1, scores_b)
            out_copy(tile).start()
            out_copy(tile + 1).start()
            return carry

        @pl.when(thirds == count)
        def _(score=score, trip=trip):
            score(0, 0, scores_a)
            lax.fori_loop(0, seeing, trip, 0)

    for tile in range(tiles):
        out_copy(tile).wait()


def body(doc_lengths, queries, key_states, value_states):
    rows, cols = queries.shape
    tiles = rows // TILE
    group_rows = HALF_HEADS * TILE
    vmem = pltpu.VMEM
    in_vmem = pl.BlockSpec(memory_space=pltpu.VMEM)
    in_hbm = pl.BlockSpec(memory_space=pltpu.HBM)
    bf16, f32 = jnp.bfloat16, jnp.float32
    state = pl.pallas_call(
        kernel,
        out_shape=(
            vmem((tiles, 2, group_rows, 2 * HD), f32),
            vmem((tiles, 2, group_rows, 128), f32),
            vmem((rows, cols), bf16),
            vmem((5, rows, HD), bf16),
            vmem((5, rows, HD), bf16),
            vmem((rows, 128), bf16),
            vmem((5, rows, 128), bf16),
            vmem((8, 128), f32),
        ),
        in_specs=[pl.BlockSpec(memory_space=pltpu.SMEM), in_hbm, in_hbm, in_hbm],
        out_specs=(in_vmem,) * 8,
        scratch_shapes=[
            vmem((2, rows // 2, HD), bf16),
            vmem((1, 1, 128), jnp.int32),
            vmem((SEQ, 1, 128), jnp.int32),
            vmem((HEADS, SEQ, 1, 128), jnp.int32),
            vmem((rows, 128), f32),
            vmem((TILE, rows), f32),
            vmem((2, 2, group_rows, 2 * TILE), f32),
            vmem((2, 2, group_rows, 4 * TILE), f32),
            vmem((2, 2, group_rows, 6 * TILE), f32),
            vmem((group_rows, rows), f32),
            vmem((group_rows, rows), f32),
            pltpu.SemaphoreType.DMA((3,)),
            pltpu.SemaphoreType.DMA((4, 2, 2)),
            pltpu.SemaphoreType.DMA((4, 2, 2)),
            pltpu.SemaphoreType.DMA((SEQ + HEADS - 2,)),
            pltpu.SemaphoreType.DMA((SEQ + HEADS - 2,)),
        ],
        compiler_params=pltpu.CompilerParams(
            collective_id=0, has_side_effects=True, vmem_limit_bytes=47 * 1024 * 1024
        ),
    )(doc_lengths, queries, key_states, value_states)
    return pl.pallas_call(
        tail,
        out_shape=jax.ShapeDtypeStruct((rows, cols), bf16),
        in_specs=[in_vmem] * 8,
        out_specs=in_hbm,
        scratch_shapes=[
            vmem((rows, cols), bf16),
            vmem((group_rows, rows), f32),
            vmem((group_rows, rows), f32),
            pltpu.SemaphoreType.DMA((tiles,)),
        ],
        compiler_params=pltpu.CompilerParams(vmem_limit_bytes=24 * 1024 * 1024),
    )(*state)


def solution(mesh):
    return jax.shard_map(
        body,
        mesh=mesh,
        in_specs=(P(("seq", "head")), P("seq", "head"), P("seq", "head"), P("seq", "head")),
        out_specs=P("seq", "head"),
        check_vma=False,
    )
```

```python
import functools
import math

import jax
import jax.numpy as jnp
from jax import lax
from jax.experimental import pallas as pl
from jax.experimental.pallas import tpu as pltpu
from jax.sharding import PartitionSpec as P

HD = 128
TILE = 128
HALF_HEADS = 4
SEQ = 32
RING = 8
HEADS = 8
LOG2_SCALE = math.log2(math.e) / math.sqrt(HD)
HIDDEN = -1e30
MESH = pl.DeviceIdType.MESH


def stacked_queries(q_buf, q_extra, tile, group):
    at = pl.ds(tile * TILE, TILE)
    parts = []
    for n in range(HALF_HEADS):
        cols = pl.ds((group * HALF_HEADS + n) * HD, HD)
        parts.append(q_buf[at, cols])
    stacked = jnp.concatenate(parts, axis=0)
    if q_extra is None:
        return stacked
    extra = jnp.concatenate([q_extra[at, :]] * HALF_HEADS, axis=0)
    return jnp.concatenate([stacked, extra], axis=1)


def dot_keys(queries, keys):
    return lax.dot_general(
        queries, keys, (((1,), (1,)), ((), ())), preferred_element_type=jnp.float32
    )


def weigh(scores, values, bias, old_max):
    width = values.shape[0]
    parts, tops, shrinks = [], [], []
    for n in range(HALF_HEADS):
        at = pl.ds(n * TILE, TILE)
        s = scores[at, pl.ds(0, width)]
        if bias is not None:
            s = s + bias[:, pl.ds(0, width)]
        top = jnp.max(s, axis=1, keepdims=True)
        if old_max is None:
            tops.append(jnp.broadcast_to(top, (TILE, 128)))
        else:
            old = old_max[at, :]
            top = jnp.maximum(old, top)
            tops.append(top)
            shrinks.append(jnp.exp2((old - top) * LOG2_SCALE))
            top = jnp.concatenate([top] * (width // 128), axis=1)
        parts.append(jnp.exp2((s - top) * LOG2_SCALE).astype(jnp.bfloat16))
    values = jnp.concatenate([values, jnp.ones((width, 128), jnp.bfloat16)], axis=1)
    update = jnp.dot(
        jnp.concatenate(parts, axis=0), values, preferred_element_type=jnp.float32
    )
    return update, tops, shrinks


def both_halves(shrinks):
    shrink = jnp.concatenate(shrinks, axis=0)
    return jnp.concatenate([shrink, shrink], axis=1)


def kernel(
    len_ref, q_hbm, k_hbm, v_hbm,
    acc, row_max, q_buf, k_buf, v_buf, q_extra, k_extra, crossing,
    relay_buf, own_len, len_seq, len_all, starts, bias,
    own_scores_0, own_scores_1, own_scores_2, scores_a, scores_b,
    load_sems, send_sems, recv_sems, len_send, len_recv,
):
    rows = q_hbm.shape[0]
    half = rows // 2
    tiles = rows // TILE
    own_scores = (own_scores_0, own_scores_1, own_scores_2)
    seq = lax.axis_index("seq")
    head = lax.axis_index("head")
    along_seq = [(lax.rem(seq + k, SEQ), head) for k in range(1, SEQ)]
    along_head = [(seq, lax.rem(head + k, HEADS)) for k in range(1, HEADS)]
    following = along_seq[0]
    ahead = lax.rem(seq + 4, SEQ)
    relay = (ahead // RING * RING + lax.rem(seq + RING - 2, RING), head)
    relayed = (seq // RING * RING + lax.rem(seq + RING - 2, RING), head)

    load_k = pltpu.make_async_copy(k_hbm, k_buf.at[0], load_sems.at[0])
    load_v = pltpu.make_async_copy(v_hbm, v_buf.at[0], load_sems.at[1])
    load_q = pltpu.make_async_copy(q_hbm, q_buf, load_sems.at[2])
    load_k.start()
    load_v.start()
    load_q.start()
    length = jnp.full((1, 1, 128), len_ref[0], jnp.int32)
    own_len[...] = length
    len_seq[pl.ds(seq, 1)] = length

    barrier = pltpu.get_barrier_semaphore()
    partners = along_seq + along_head
    for partner in partners:
        pl.semaphore_signal(barrier, inc=1, device_id=partner, device_id_type=MESH)
    pl.semaphore_wait(barrier, len(partners))

    def sends(source, target, partners_of, base):
        return [
            pltpu.make_async_remote_copy(
                src_ref=source, dst_ref=target,
                send_sem=len_send.at[base + n], recv_sem=len_recv.at[base + n],
                device_id=partner, device_id_type=MESH,
            )
            for n, partner in enumerate(partners_of)
        ]

    def hop(slot, part):
        at = pl.ds(part * half, half)
        if slot < 3:
            pairs = [(buf.at[slot, at], buf.at[slot + 1, at]) for buf in (k_buf, v_buf)]
            target = following
        elif part == 0:
            late = pl.ds(half, half)
            pairs = [(buf.at[0, late], relay_buf.at[n]) for n, buf in enumerate((k_buf, v_buf))]
            target = relay
        else:
            early = pl.ds(0, half)
            pairs = [(relay_buf.at[n], buf.at[4, early]) for n, buf in enumerate((k_buf, v_buf))]
            target = relayed
        return [
            pltpu.make_async_remote_copy(
                src_ref=source, dst_ref=held,
                send_sem=send_sems.at[slot, part, n], recv_sem=recv_sems.at[slot, part, n],
                device_id=target, device_id_type=MESH,
            )
            for n, (source, held) in enumerate(pairs)
        ]

    hops = {(slot, part): hop(slot, part) for slot in range(4) for part in range(2)}

    def start_hop(slot, part):
        for copy in hops[slot, part]:
            copy.start()

    def wait_hop(slot, part):
        for copy in hops[slot, part]:
            copy.wait_recv()

    def arrived(slot, part):
        wait_hop(slot, part)
        if slot < 2:
            start_hop(slot + 1, part)

    seq_sends = sends(own_len, len_seq.at[pl.ds(seq, 1)], along_seq, 0)
    for copy in seq_sends:
        copy.start()
    load_k.wait()
    load_v.wait()
    start_hop(0, 0)
    start_hop(0, 1)
    start_hop(3, 0)
    load_q.wait()
    for tile in range(tiles):
        pair = tile // 2
        for group in range(2):
            own_scores[pair][tile % 2, group] = dot_keys(
                stacked_queries(q_buf, None, tile, group),
                k_buf[0, pl.ds(0, 2 * TILE * (pair + 1)), :],
            )
    for copy in seq_sends:
        copy.wait_recv()
    head_sends = sends(len_seq, len_all.at[head], along_head, SEQ - 1)
    for copy in head_sends:
        copy.start()
    len_all[pl.ds(head, 1)] = len_seq[...].reshape(1, SEQ, 1, 128)
    arrived(0, 0)
    for copy in head_sends:
        copy.wait_recv()
    arrived(0, 1)

    lane = lax.broadcasted_iota(jnp.int32, (1, 128), 1)

    def add_lengths(n, ends):
        low, high = ends
        for m in range(HEADS):
            length_row = len_all[m, n]
            doc = n * HEADS + m
            low = low + jnp.where(lane >= doc, length_row, 0)
            high = high + jnp.where(lane + 128 >= doc, length_row, 0)
        return low, high

    zero_row = jnp.zeros((1, 128), jnp.int32)
    low, high = lax.fori_loop(0, SEQ, add_lengths, (zero_row, zero_row))
    first = seq * rows
    ends = (jnp.concatenate([low, high], axis=1) - first).astype(jnp.float32)
    far = float(1 << 24)
    doc_first = jnp.max(
        jnp.maximum(jnp.where(ends <= 0, ends, -far), (0 - first).astype(jnp.float32)),
        axis=1, keepdims=True,
    )
    doc_end = jnp.min(jnp.where(ends > 0, ends, far), axis=1, keepdims=True)
    crossing[0:1, :] = jnp.broadcast_to(doc_first, (1, 128))
    crossing[1:2, :] = jnp.broadcast_to(doc_end, (1, 128))
    column = lax.broadcasted_iota(jnp.int32, (TILE, 128), 0).astype(jnp.float32)
    lanes = lax.broadcasted_iota(jnp.int32, (TILE, 128), 1)
    unseen_lane = jnp.where(lanes == 0, HIDDEN, 0.0)
    one_lane = jnp.where(lanes == 1, 1.0, 0.0)
    for tile in range(tiles):
        at = pl.ds(tile * TILE, TILE)
        position = column + float(tile * TILE)
        done = jnp.where(ends <= position[:, :1], ends, -far)
        starts[at, :] = jnp.broadcast_to(jnp.max(done, axis=1, keepdims=True), (TILE, 128))
        later = (lanes == 0) & (position >= doc_end)
        q_extra[at, :] = jnp.where(later, 1.0, one_lane).astype(jnp.bfloat16)
        for slot in range(1, 5):
            before = (lanes == 1) & (position < doc_first + float(slot * rows))
            k_extra[slot, at, :] = jnp.where(before, HIDDEN, unseen_lane).astype(jnp.bfloat16)

    def score(slot, keys_at, extra_at, tile, group, target):
        keys = jnp.concatenate([k_buf[slot, keys_at, :], k_extra[slot, extra_at, :]], axis=1)
        target[:, pl.ds(0, keys_at.size)] = dot_keys(
            stacked_queries(q_buf, q_extra, tile, group), keys
        )

    def combine(slot, keys_at, tile, group, source):
        update, tops, shrinks = weigh(
            source, v_buf[slot, keys_at, :], None, row_max.at[tile, group]
        )
        for n, top in enumerate(tops):
            row_max[tile, group, pl.ds(n * TILE, TILE), :] = top
        acc[tile, group] = acc[tile, group] * both_halves(shrinks) + update

    for tile in range(tiles):
        pair = tile // 2
        width = 2 * TILE * (pair + 1)
        token = lax.broadcasted_iota(jnp.int32, (TILE, width), 1)
        mine = tile * TILE + lax.broadcasted_iota(jnp.int32, (TILE, width), 0)
        begins = starts[pl.ds(tile * TILE, TILE), :]
        begins = jnp.concatenate([begins] * (width // 128), axis=1)
        seen = (token.astype(jnp.float32) >= begins) & (token <= mine)
        bias[:, pl.ds(0, width)] = jnp.where(seen, 0.0, HIDDEN)
        for group in range(2):
            update, tops, _ = weigh(
                own_scores[pair].at[tile % 2, group], v_buf[0, pl.ds(0, width), :], bias, None
            )
            for n, top in enumerate(tops):
                row_max[tile, group, pl.ds(n * TILE, TILE), :] = top
            acc[tile, group] = update
        if tile == 1:
            wait_hop(3, 0)
            start_hop(3, 1)

    whole = pl.ds(0, rows)
    step = 3
    blocks = tiles // step
    trips = 2 * blocks
    buffers = (scores_a, scores_b)

    def place(trip):
        return trip // blocks + 1, trip % blocks * step

    def trip_body(trip, carry):
        for when, slot, part in ((0, 1, 0), (1, 1, 1), (3, 2, 0)):
            pl.when(trip == when)(functools.partial(arrived, slot, part))
        slot, tile = place(trip)
        next_slot, next_tile = place(jnp.minimum(trip + 1, trips - 1))
        units = [(slot, tile + n, group) for n in range(step) for group in range(2)]
        for n, (_, at_tile, group) in enumerate(units):
            ahead_slot, ahead_tile, ahead_group = (units + [(next_slot, next_tile, 0)])[n + 1]
            score(ahead_slot, whole, whole, ahead_tile, ahead_group, buffers[1 - n % 2])
            combine(slot, whole, at_tile, group, buffers[n % 2])
        return carry

    score(1, whole, whole, 0, 0, scores_a)
    lax.fori_loop(0, trips, trip_body, 0)
    wait_hop(3, 1)
    wait_hop(2, 1)
    for copy in seq_sends + head_sends:
        copy.wait_send()
    for copies in hops.values():
        for copy in copies:
            copy.wait_send()


def tail(
    acc, row_max, q_buf, k_buf, v_buf, q_extra, k_extra, crossing, out_hbm,
    out_buf, scores_a, scores_b, sems,
):
    rows = q_buf.shape[0]
    tiles = rows // TILE
    third, half = rows // 3, rows // 2
    doc_first = jnp.max(crossing[0:1, :]).astype(jnp.int32)
    doc_end = jnp.max(crossing[1:2, :]).astype(jnp.int32)
    first_key = doc_first + 3 * rows
    thirds = 3 - jnp.clip(first_key // third, 0, 3)
    variant = jnp.where(first_key < 0, 4, thirds)
    seeing = (jnp.minimum(doc_end, rows) + TILE - 1) // TILE
    seeing = jnp.where(variant > 0, seeing, 0)

    def out_copy(tile):
        at = pl.ds(tile * TILE, TILE)
        return pltpu.make_async_copy(out_buf.at[at], out_hbm.at[at], sems.at[tile])

    def put(tile, group, total):
        total = (total[:, :HD] / total[:, HD:]).astype(jnp.bfloat16)
        for n in range(HALF_HEADS):
            cols = pl.ds((group * HALF_HEADS + n) * HD, HD)
            out_buf[pl.ds(tile * TILE, TILE), cols] = total[n * TILE : (n + 1) * TILE]

    def finish(tile, carry):
        for group in range(2):
            put(tile, group, acc[tile, group])
        out_copy(tile).start()
        return carry

    lax.fori_loop(seeing, tiles, finish, 0)

    for count in range(1, 5):
        key0 = max(rows - count * third, 0)
        pieces = [(3, pl.ds(key0, rows - key0), pl.ds(key0, rows - key0))]
        if count == 4:
            pieces.append((4, pl.ds(0, half), pl.ds(half, half)))

        def score(tile, group, target, pieces=pieces):
            keys = jnp.concatenate(
                [
                    jnp.concatenate([k_buf[slot, at, :], k_extra[slot, extra_at, :]], axis=1)
                    for slot, at, extra_at in pieces
                ],
                axis=0,
            )
            target[:, pl.ds(0, keys.shape[0])] = dot_keys(
                stacked_queries(q_buf, q_extra, tile, group), keys
            )

        def combine(tile, group, source, pieces=pieces):
            values = jnp.concatenate([v_buf[slot, at, :] for slot, at, _ in pieces], axis=0)
            update, _, shrinks = weigh(source, values, None, row_max.at[tile, group])
            put(tile, group, acc[tile, group] * both_halves(shrinks) + update)

        def trip(n, carry, score=score, combine=combine):
            tile = 2 * n
            score(tile, 1, scores_b)
            combine(tile, 0, scores_a)
            score(tile + 1, 0, scores_a)
            combine(tile, 1, scores_b)
            score(tile + 1, 1, scores_b)
            combine(tile + 1, 0, scores_a)
            score(jnp.minimum(tile + 2, tiles - 1), 0, scores_a)
            combine(tile + 1, 1, scores_b)
            out_copy(tile).start()
            out_copy(tile + 1).start()
            return carry

        def odd(n, carry, score=score, combine=combine):
            score(n, 1, scores_b)
            combine(n, 0, scores_a)
            combine(n, 1, scores_b)
            out_copy(n).start()
            return carry

        @pl.when(variant == count)
        def _(score=score, trip=trip, odd=odd):
            score(0, 0, scores_a)
            lax.fori_loop(0, seeing // 2, trip, 0)
            lax.fori_loop(seeing // 2 * 2, seeing, odd, 0)

    for tile in range(tiles):
        out_copy(tile).wait()


def body(doc_lengths, queries, key_states, value_states):
    rows, cols = queries.shape
    tiles = rows // TILE
    group_rows = HALF_HEADS * TILE
    vmem = pltpu.VMEM
    in_vmem = pl.BlockSpec(memory_space=pltpu.VMEM)
    in_hbm = pl.BlockSpec(memory_space=pltpu.HBM)
    bf16, f32 = jnp.bfloat16, jnp.float32
    state = pl.pallas_call(
        kernel,
        out_shape=(
            vmem((tiles, 2, group_rows, 2 * HD), f32),
            vmem((tiles, 2, group_rows, 128), f32),
            vmem((rows, cols), bf16),
            vmem((5, rows, HD), bf16),
            vmem((5, rows, HD), bf16),
            vmem((rows, 128), bf16),
            vmem((5, rows, 128), bf16),
            vmem((8, 128), f32),
        ),
        in_specs=[pl.BlockSpec(memory_space=pltpu.SMEM), in_hbm, in_hbm, in_hbm],
        out_specs=(in_vmem,) * 8,
        scratch_shapes=[
            vmem((2, rows // 2, HD), bf16),
            vmem((1, 1, 128), jnp.int32),
            vmem((SEQ, 1, 128), jnp.int32),
            vmem((HEADS, SEQ, 1, 128), jnp.int32),
            vmem((rows, 128), f32),
            vmem((TILE, rows), f32),
            vmem((2, 2, group_rows, 2 * TILE), f32),
            vmem((2, 2, group_rows, 4 * TILE), f32),
            vmem((2, 2, group_rows, 6 * TILE), f32),
            vmem((group_rows, rows), f32),
            vmem((group_rows, rows), f32),
            pltpu.SemaphoreType.DMA((3,)),
            pltpu.SemaphoreType.DMA((4, 2, 2)),
            pltpu.SemaphoreType.DMA((4, 2, 2)),
            pltpu.SemaphoreType.DMA((SEQ + HEADS - 2,)),
            pltpu.SemaphoreType.DMA((SEQ + HEADS - 2,)),
        ],
        compiler_params=pltpu.CompilerParams(
            collective_id=0, has_side_effects=True, vmem_limit_bytes=47 * 1024 * 1024
        ),
    )(doc_lengths, queries, key_states, value_states)
    return pl.pallas_call(
        tail,
        out_shape=jax.ShapeDtypeStruct((rows, cols), bf16),
        in_specs=[in_vmem] * 8,
        out_specs=in_hbm,
        scratch_shapes=[
            vmem((rows, cols), bf16),
            vmem((group_rows, rows + rows // 2), f32),
            vmem((group_rows, rows + rows // 2), f32),
            pltpu.SemaphoreType.DMA((tiles,)),
        ],
        compiler_params=pltpu.CompilerParams(vmem_limit_bytes=24 * 1024 * 1024),
    )(*state)


def solution(mesh):
    return jax.shard_map(
        body,
        mesh=mesh,
        in_specs=(P(("seq", "head")), P("seq", "head"), P("seq", "head"), P("seq", "head")),
        out_specs=P("seq", "head"),
        check_vma=False,
    )
```
